32 devices in a mesh: leaf: 8 (over z, x), blk: 4 (over y, core).
Axes of the slice: x: 2, y: 2, z: 4, core: 2. Of those that a mesh axis runs over, the one named last changes fastest.
Arguments:
- desc_panel: bfloat16 [256, 384, 128], P(('leaf', 'blk')), may hold values from -18 to 18
- row_map: int32 [256, 3], P(('leaf', 'blk')), may hold values from 0 to 55, as said below
- anc_order: int32 [8], replicated, may hold values from 0 to 7, as said below
- anc_below: int32 [8, 12], replicated, may hold values from 32 to 55, as said below
- anc_panel: float32 [8, 4, 4, 128, 512], P('leaf', None, 'blk'), may hold values from -6 to 27, as said below
Outputs:
- chol_panel: float32 [8, 4, 4, 128, 512], P('leaf', None, 'blk')
The draws below stay inside these ranges and needn't reach their ends.
Inputs may be any that keep to these rules, and one draw needn't show every extreme that they name: `row_map`: entry 0 of each row is a column block of one ancestor; the other entries are distinct entries of that ancestor's row of anc_below. Over the descendants of one device, entry 0 names the column blocks of any one ancestor at most 2 times, and of some ancestor exactly 2 times. `anc_order`: each leaf index holds a different column range. `anc_below`: each row holds 12 distinct indices. `anc_panel`: the leading 512 rows of each ancestor's panel are symmetric, and the leading block of S stays positive definite.
All inputs are finite; a program needn't handle non-finite values.
Results may differ from the reference program's by a relative error of at most 0.0003.
Values may be sent and summed in bfloat16 or wider, within the bound.
A program may use at most 192 MiB of HBM per device.

```python
import jax
import jax.numpy as jnp
from jax import lax

BR = 128
WD = 128
CB = 4
W = 512
Q = 12
P_SIZE = 16
EXTRA = 24
RB = 3
NA = 8
DESC_DEV = 8
ND = 256
N_BLK = 4


def tree_structure(key):
    keys = jax.random.split(jax.random.fold_in(key, 41), 5)
    anc_order = jax.random.permutation(keys[0], NA).astype(jnp.int32)
    below_picks = jax.vmap(lambda k: jax.random.permutation(k, EXTRA)[:Q])(jax.random.split(keys[1], NA))
    anc_below = (below_picks + NA * CB).astype(jnp.int32)
    device_count = ND // DESC_DEV
    quarter = NA // 4

    def device_targets(k):
        first_key, second_key = jax.random.split(k)
        order = jax.random.permutation(first_key, NA)
        listed = jnp.concatenate([order[:quarter], order[:quarter], order[quarter:3 * quarter]])
        return listed[jax.random.permutation(second_key, DESC_DEV)]
    targets = jax.vmap(device_targets)(jax.random.split(keys[2], device_count)).reshape(ND).astype(jnp.int32)
    columns = jax.random.randint(keys[3], (ND,), 0, CB).astype(jnp.int32)
    picks = jax.vmap(lambda k: jax.random.permutation(k, Q)[:RB - 1])(jax.random.split(keys[4], ND)).astype(jnp.int32)
    below = jnp.take_along_axis(anc_below[targets], picks, axis=1)
    head = anc_order[targets] * CB + columns
    row_map = jnp.concatenate([head[:, None], below], axis=1).astype(jnp.int32)
    return (anc_order, anc_below, row_map)


def draw_anc_order(key, part):
    return tree_structure(key)[0]


def draw_anc_below(key, part):
    return tree_structure(key)[1]


def draw_row_map(key, part):
    return tree_structure(key)[2]


def draw_desc_panel(key, part):
    key = jax.random.fold_in(key, 31)
    shape = (ND, RB, BR, WD)
    values = jnp.clip(jax.random.normal(key, shape, jnp.float32), -6.0, 6.0)
    device_count = ND // DESC_DEV
    head_scale = (2.0 * CB / (device_count * WD)) ** 0.5
    scales = jnp.where(jnp.arange(RB) < 1, head_scale, 3.0).astype(jnp.float32)
    return (values * scales[None, :, None, None]).reshape(ND, RB * BR, WD).astype(jnp.bfloat16)


def draw_anc_panel(key, part):
    keys = jax.random.split(jax.random.fold_in(key, 23), 2)
    total_rows = P_SIZE * BR
    noise = jnp.clip(jax.random.normal(keys[0], (NA, total_rows, W), jnp.float32), -6.0, 6.0)
    diagonal = jax.random.uniform(keys[1], (NA, W), jnp.float32, 12.0, 24.0)
    upper = noise[:, :W, :] * (1.5 / W ** 0.5)
    symmetric = (upper + jnp.swapaxes(upper, 1, 2)) / 2.0 ** 0.5
    symmetric = symmetric + diagonal[:, :, None] * jnp.eye(W, dtype=jnp.float32)[None, :, :]
    whole = jnp.concatenate([symmetric, noise[:, W:, :]], axis=1)
    return whole.reshape(NA, P_SIZE // N_BLK, N_BLK, BR, W).astype(jnp.float32)


def setup_inputs(seed: int = 0) -> dict:
    seeds = jax.random.split(jax.random.key(seed), 6)
    return {
        "desc_panel": draw_desc_panel(jax.random.fold_in(seeds[5], 71), 0),
        "row_map": draw_row_map(jax.random.fold_in(seeds[5], 71), 0),
        "anc_order": draw_anc_order(jax.random.fold_in(seeds[5], 71), 0),
        "anc_below": draw_anc_below(jax.random.fold_in(seeds[5], 71), 0),
        "anc_panel": draw_anc_panel(jax.random.fold_in(seeds[5], 71), 0),
    }


def structure_positions(block_ids, owner_leaf, anc_order, anc_below):
    column_base = anc_order[owner_leaf] * CB
    relative = block_ids - column_base[:, None]
    in_columns = (relative >= 0) & (relative < CB)
    below_ids = anc_below[owner_leaf]
    matching = block_ids[:, :, None] == below_ids[:, None, :]
    offsets = CB + jnp.arange(Q, dtype=jnp.int32)
    below_place = jnp.sum(jnp.where(matching, offsets[None, None, :], 0), axis=2)
    located = jnp.any(matching, axis=2)
    return jnp.where(in_columns, relative, jnp.where(located, below_place, P_SIZE)).astype(jnp.int32)

def owner_of(ranges, anc_order):
    leaves = jnp.arange(NA, dtype=jnp.int32)
    return jnp.sum(jnp.where(anc_order[None, :] == ranges[:, None], leaves[None, :], 0), axis=1).astype(jnp.int32)

def reference(desc_panel, row_map, anc_order, anc_below, anc_panel):
    device_count = ND // DESC_DEV
    panel_groups = desc_panel.reshape(device_count, DESC_DEV, RB, BR, WD)
    id_groups = row_map.reshape(device_count, DESC_DEV, RB)

    def absorb(running, element):
        panel_block, block_ids = element
        blocks = panel_block.astype(jnp.float32)
        owner_leaf = owner_of(block_ids[:, 0] // CB, anc_order)
        positions = structure_positions(block_ids, owner_leaf, anc_order, anc_below)
        column = (block_ids[:, 0] % CB).astype(jnp.int32)
        product = jnp.einsum('nrxw,nyw->nrxy', blocks, blocks[:, 0], precision=lax.Precision.HIGHEST)
        running = running.at[owner_leaf[:, None], positions, :, column[:, None], :].add(product)
        return (running, None)
    initial = jnp.zeros((NA, P_SIZE + 1, BR, CB, BR), jnp.float32)
    running, _ = lax.scan(absorb, initial, (panel_groups, id_groups))
    update = running[:, :P_SIZE].reshape(NA, P_SIZE * BR, W)
    schur_rows = anc_panel.reshape(NA, P_SIZE * BR, W) - update

    def factor(panel_rows):
        lower_factor = jnp.linalg.cholesky(panel_rows[:W])
        return jax.scipy.linalg.solve_triangular(lower_factor, panel_rows.T, lower=True).T
    return lax.map(factor, schur_rows).reshape(anc_panel.shape)
```

```python
import jax
import jax.numpy as jnp
from jax import lax
from jax.experimental import pallas as pl
from jax.experimental.pallas import tpu as pltpu
from jax.sharding import PartitionSpec as P

SLOTS = 2

GROUP = 16


def split(x):
    hi = x.astype(jnp.bfloat16)
    return hi, (x - hi.astype(jnp.float32)).astype(jnp.bfloat16)


def dot_rows(lhs, rhs):
    lhs_hi, lhs_lo = lhs
    rhs_hi, rhs_lo = rhs
    return lax.dot_general(
        jnp.concatenate([lhs_hi, lhs_lo, lhs_hi], axis=0),
        jnp.concatenate([rhs_hi, rhs_hi, rhs_lo], axis=0),
        (((0,), (0,)), ((), ())),
        preferred_element_type=jnp.float32,
    )


def factor_strip(strip):
    tiles, rows, _ = strip.shape
    sub = lax.broadcasted_iota(jnp.int32, (GROUP, rows), 0)
    for g in range(rows // GROUP):
        r0 = g * GROUP
        held = [strip[q, r0 : r0 + GROUP, :] for q in range(tiles)]
        cols = [
            jnp.broadcast_to(held[0][:, r0 + t : r0 + t + 1], (GROUP, rows)) for t in range(GROUP)
        ]
        scale = jnp.zeros((GROUP, rows), jnp.float32)
        for t in range(GROUP):
            root = lax.rsqrt(cols[t][t : t + 1, :])
            scale = jnp.where(sub == t, root, scale)
            if t < GROUP - 1:
                mult = jnp.where(sub > t, cols[t], 0.0) * (root * root)
                for u in range(t + 1, GROUP):
                    cols[u] = cols[u] - mult * cols[u][t : t + 1, :]
                held = [h - mult * h[t : t + 1, :] for h in held]
        held = [h * scale for h in held]
        for q in range(tiles):
            strip[q, r0 : r0 + GROUP, :] = held[q]
        if r0 + GROUP < rows:
            pieces = [split(h) for h in held]
            rhs = tuple(jnp.concatenate([p[n] for p in pieces], axis=1) for n in range(2))
            drop = dot_rows(pieces[0], rhs)
            for q in range(tiles):
                strip[q, r0 + GROUP :, :] = (
                    strip[q, r0 + GROUP :, :] - drop[r0 + GROUP :, q * rows : (q + 1) * rows]
                )


def factor_kernel(top, own, other, upper, inverse, work, strip):
    blocks, rows = top.shape[0], top.shape[1]
    for j in range(blocks):
        for k in range(blocks):
            tile = top[j, :, k * rows : (k + 1) * rows]
            if j == k:
                tile = tile - own[k]
                for n in range(other.shape[0]):
                    tile = tile - other[n, k]
            work[j, k] = tile
    line = lax.broadcasted_iota(jnp.int32, (rows, rows), 0)
    lane = lax.broadcasted_iota(jnp.int32, (rows, rows), 1)

    def step(k, carry):
        strip[0] = work[k, k]
        strip[1] = jnp.where(line == lane, 1.0, 0.0)
        for q in range(1, blocks):
            strip[1 + q] = work[k, lax.rem(k + q, blocks)]
        factor_strip(strip)
        upper[k, k] = jnp.where(lane >= line, strip[0], 0.0)
        inverse[k, k] = strip[1]
        for q in range(1, blocks):
            j = lax.rem(k + q, blocks)
            ahead = k + q < blocks
            upper[k, j] = jnp.where(ahead, strip[1 + q], 0.0)
            inverse[k, j] = jnp.where(ahead, 0.0, strip[1 + q])
        pieces = [split(strip[1 + q]) for q in range(blocks)]
        rhs = tuple(jnp.concatenate([p[n] for p in pieces], axis=1) for n in range(2))
        for ahead in range(1, blocks):

            @pl.when(k + ahead < blocks)
            def _():
                j = k + ahead
                drop = dot_rows(split(strip[1 + ahead]), rhs)
                work[j, k] = -drop[:, :rows]
                for q in range(1, blocks):
                    at = lax.rem(k + q, blocks)
                    work[j, at] = work[j, at] - drop[:, q * rows : (q + 1) * rows]

        return carry

    lax.fori_loop(0, blocks, step, 0)


def factor(top, own, other):
    blocks, rows = top.shape[0], top.shape[1]
    square = jax.ShapeDtypeStruct((blocks, blocks, rows, rows), jnp.float32)
    return pl.pallas_call(
        factor_kernel,
        out_shape=(square, square),
        in_specs=[pl.BlockSpec(memory_space=pltpu.VMEM)] * 3,
        out_specs=(pl.BlockSpec(memory_space=pltpu.VMEM),) * 2,
        scratch_shapes=[
            pltpu.VMEM((blocks, blocks, rows, rows), jnp.float32),
            pltpu.VMEM((blocks + 1, rows, rows), jnp.float32),
        ],
        cost_estimate=pl.CostEstimate(
            flops=2 * (blocks * rows) ** 3, bytes_accessed=64 * 1024 * 1024, transcendentals=0
        ),
        name="factor",
    )(top, own, other)


def update_kernel(parity, codes, mine, theirs, diag, below):
    slots = mine.shape[0]
    rows = mine.shape[2]
    halves, per_dest, columns = below.shape[0], below.shape[1], below.shape[2]
    pair = 2
    blk_count = halves * pair
    position_count = (per_dest + 1) * blk_count
    block_count = mine.shape[1] // rows
    diag[...] = jnp.zeros_like(diag)
    below[...] = jnp.zeros_like(below)

    for half, source in enumerate((mine, theirs)):

        def absorb(s, carry, half=half, source=source):
            column = codes[half, s * block_count]

            @pl.when(column < position_count)
            def _():
                panel = source[s]
                product = lax.dot_general(
                    panel,
                    panel[:rows],
                    (((1,), (1,)), ((), ())),
                    preferred_element_type=jnp.float32,
                )
                diag[column] += product[:rows]
                for r in range(1, block_count):
                    place = codes[half, s * block_count + r]
                    dest = lax.rem(place, blk_count)

                    @pl.when((lax.rem(dest, pair) == parity[0]) & (place < position_count))
                    def _():
                        at = (lax.div(dest, pair), lax.div(place, blk_count) - 1, column)
                        below[at] += product[r * rows : (r + 1) * rows]

            return carry

        lax.fori_loop(0, slots, absorb, 0)


def local_update(parity, codes, mine, theirs, blk_count, columns, per_dest):
    rows = mine.shape[2]
    smem = pl.BlockSpec(memory_space=pltpu.SMEM)
    vmem = pl.BlockSpec(memory_space=pltpu.VMEM)
    return pl.pallas_call(
        update_kernel,
        out_shape=(
            jax.ShapeDtypeStruct((columns, rows, rows), jnp.float32),
            jax.ShapeDtypeStruct((blk_count // 2, per_dest, columns, rows, rows), jnp.float32),
        ),
        in_specs=[smem, smem, vmem, vmem],
        out_specs=(vmem, vmem),
        cost_estimate=pl.CostEstimate(
            flops=4 * mine.size * rows, bytes_accessed=8 * mine.size, transcendentals=0
        ),
        name="update",
    )(parity, codes, mine, theirs)


def finish_kernel(me, panel, own, other, upper, inverse, out):
    per_dest, rows = own.shape[0], own.shape[2]
    blocks = upper.shape[0]
    for k in range(blocks):
        tile = upper[k, me[0]]
        out[0, :, k * rows : (k + 1) * rows] = tile.T
    left = []
    for i in range(per_dest):
        parts = []
        for k in range(blocks):
            tile = panel[i + 1, :, k * rows : (k + 1) * rows] - own[i, k]
            for n in range(other.shape[0]):
                tile = tile - other[n, i, k]
            parts.append(tile)
        left.append(jnp.concatenate(parts, axis=1))
    whole_hi, whole_lo = split(jnp.concatenate(left, axis=0))
    for k in range(blocks):
        wide = (k + 1) * rows
        right = jnp.concatenate([inverse[k, q] for q in range(k + 1)], axis=1)
        right_hi, right_lo = split(right)

        def times(x, y):
            return lax.dot_general(
                x, y, (((1,), (1,)), ((), ())), preferred_element_type=jnp.float32
            )

        solved = (
            times(whole_hi[:, :wide], right_hi)
            + times(whole_lo[:, :wide], right_hi)
            + times(whole_hi[:, :wide], right_lo)
        )
        for i in range(per_dest):
            out[i + 1, :, k * rows : (k + 1) * rows] = solved[i * rows : (i + 1) * rows]


def finish(me, panel, own, other, upper, inverse):
    smem = pl.BlockSpec(memory_space=pltpu.SMEM)
    vmem = pl.BlockSpec(memory_space=pltpu.VMEM)
    return pl.pallas_call(
        finish_kernel,
        out_shape=jax.ShapeDtypeStruct(panel.shape, panel.dtype),
        in_specs=[smem] + [vmem] * 5,
        out_specs=vmem,
        cost_estimate=pl.CostEstimate(
            flops=6 * panel.size * panel.shape[2], bytes_accessed=8 * panel.size, transcendentals=0
        ),
        name="finish",
    )(me, panel, own, other, upper, inverse)


def leaf_owner(ranges, anc_order):
    leaves = jnp.arange(anc_order.shape[0], dtype=jnp.int32)
    return jnp.sum(jnp.where(anc_order[None, :] == ranges[:, None], leaves[None, :], 0), axis=1)


def block_positions(block_ids, owner_leaf, anc_order, anc_below, column_blocks, position_count):
    column_base = anc_order[owner_leaf] * column_blocks
    relative = block_ids - column_base[:, None]
    in_columns = (relative >= 0) & (relative < column_blocks)
    below_ids = anc_below[owner_leaf]
    matching = block_ids[:, :, None] == below_ids[:, None, :]
    offsets = column_blocks + jnp.arange(below_ids.shape[1], dtype=jnp.int32)
    below_place = jnp.sum(jnp.where(matching, offsets[None, None, :], 0), axis=2)
    located = jnp.any(matching, axis=2)
    return jnp.where(in_columns, relative, jnp.where(located, below_place, position_count))


def shards(desc_panel, row_map, anc_order, anc_below, anc_panel):
    leaf_count = lax.axis_size("leaf")
    blk_count = lax.axis_size("blk")
    desc_count, block_count = row_map.shape
    block_rows = anc_panel.shape[3]
    panel_width = anc_panel.shape[4]
    wide_desc = desc_panel.shape[2]
    column_blocks = panel_width // block_rows
    position_count = column_blocks + anc_below.shape[1]
    if column_blocks != blk_count or blk_count % 2 or wide_desc != block_rows:
        raise ValueError("unsupported sizes")
    slot_count = leaf_count * SLOTS
    mine = lax.axis_index("blk")
    swap = [(b, b ^ 1) for b in range(blk_count)]

    def shift(x, by):
        return lax.ppermute(x, "blk", [(b, (b + by) % blk_count) for b in range(blk_count)])

    local_rows = anc_panel.reshape(anc_panel.shape[1], block_rows, panel_width)
    own_top = local_rows[0]
    tops = [own_top] + [shift(own_top, by) for by in range(1, blk_count)]
    top = jnp.stack(tops)[(mine - jnp.arange(blk_count)) % blk_count]

    owner_leaf = leaf_owner(row_map[:, 0] // column_blocks, anc_order)
    positions = block_positions(
        row_map, owner_leaf, anc_order, anc_below, column_blocks, position_count
    )
    desc_index = jnp.arange(desc_count, dtype=jnp.int32)
    same_owner = owner_leaf[:, None] == owner_leaf[None, :]
    earlier = desc_index[None, :] < desc_index[:, None]
    ranking = jnp.sum(same_owner & earlier, axis=1)
    slot_of = owner_leaf * SLOTS + ranking
    matches = slot_of[None, :] == jnp.arange(slot_count, dtype=jnp.int32)[:, None]
    filled = jnp.any(matches, axis=1)
    chosen = jnp.sum(jnp.where(matches, desc_index[None, :], 0), axis=1)
    slot_codes = jnp.where(filled[:, None], positions[chosen], position_count).reshape(
        leaf_count, SLOTS * block_count
    )
    send_rows = jnp.take(desc_panel, chosen, axis=0)
    send_rows = send_rows.reshape(leaf_count, SLOTS, block_count * block_rows, wide_desc)
    received = lax.all_to_all(send_rows, "leaf", split_axis=0, concat_axis=0, tiled=True)
    codes = lax.all_to_all(
        slot_codes.astype(jnp.bfloat16), "leaf", split_axis=0, concat_axis=0, tiled=True
    )
    received = received.reshape(slot_count, block_count * block_rows, wide_desc)
    codes = codes.reshape(1, slot_count * block_count)
    their_rows = lax.ppermute(received, "blk", swap)
    their_codes = lax.ppermute(codes, "blk", swap)
    both_codes = jnp.concatenate([codes, their_codes], axis=0).astype(jnp.int32)

    per_dest = local_rows.shape[0] - 1
    parity = (mine % 2).astype(jnp.int32).reshape(1)
    diag, below = local_update(
        parity, both_codes, received, their_rows, blk_count, column_blocks, per_dest
    )
    half = blk_count // 2
    here = mine // 2
    steps = range(1, half)
    other_diag = jnp.stack([shift(diag, 2 * s) for s in steps])
    other_below = jnp.stack(
        [shift(lax.dynamic_index_in_dim(below, (here + s) % half, 0, False), 2 * s) for s in steps]
    )
    own_below = lax.dynamic_index_in_dim(below, here, 0, False)
    upper, inverse = factor(top, diag, other_diag)
    me = mine.astype(jnp.int32).reshape(1)
    out = finish(me, local_rows, own_below, other_below, upper, inverse)
    return out.reshape(anc_panel.shape)


def solution(mesh):
    in_specs = (
        P(("leaf", "blk"), None, None),
        P(("leaf", "blk"), None),
        P(),
        P(),
        P("leaf", None, "blk", None, None),
    )
    out_specs = P("leaf", None, "blk", None, None)
    return jax.shard_map(shards, mesh=mesh, in_specs=in_specs, out_specs=out_specs, check_vma=False)
```

```python
import jax
import jax.numpy as jnp
from jax import lax
from jax.experimental import pallas as pl
from jax.experimental.pallas import tpu as pltpu
from jax.sharding import PartitionSpec as P

SLOTS = 2
PAIR = 2

GROUP = 16


def split(x):
    hi = x.astype(jnp.bfloat16)
    return hi, (x - hi.astype(jnp.float32)).astype(jnp.bfloat16)


def dot_rows(lhs, rhs):
    lhs_hi, lhs_lo = lhs
    rhs_hi, rhs_lo = rhs
    return lax.dot_general(
        jnp.concatenate([lhs_hi, lhs_lo, lhs_hi], axis=0),
        jnp.concatenate([rhs_hi, rhs_hi, rhs_lo], axis=0),
        (((0,), (0,)), ((), ())),
        preferred_element_type=jnp.float32,
    )


def factor_strip(strip):
    tiles, rows, _ = strip.shape
    sub = lax.broadcasted_iota(jnp.int32, (GROUP, rows), 0)
    for g in range(rows // GROUP):
        r0 = g * GROUP
        held = [strip[q, r0 : r0 + GROUP, :] for q in range(tiles)]
        cols = [
            jnp.broadcast_to(held[0][:, r0 + t : r0 + t + 1], (GROUP, rows)) for t in range(GROUP)
        ]
        scale = jnp.zeros((GROUP, rows), jnp.float32)
        for t in range(GROUP):
            root = lax.rsqrt(cols[t][t : t + 1, :])
            scale = jnp.where(sub == t, root, scale)
            if t < GROUP - 1:
                mult = jnp.where(sub > t, cols[t], 0.0) * (root * root)
                for u in range(t + 1, GROUP):
                    cols[u] = cols[u] - mult * cols[u][t : t + 1, :]
                held = [h - mult * h[t : t + 1, :] for h in held]
        held = [h * scale for h in held]
        for q in range(tiles):
            strip[q, r0 : r0 + GROUP, :] = held[q]
        if r0 + GROUP < rows:
            pieces = [split(h) for h in held]
            rhs = tuple(jnp.concatenate([p[n] for p in pieces], axis=1) for n in range(2))
            drop = dot_rows(pieces[0], rhs)
            for q in range(tiles):
                strip[q, r0 + GROUP :, :] = (
                    strip[q, r0 + GROUP :, :] - drop[r0 + GROUP :, q * rows : (q + 1) * rows]
                )


def factor_kernel(top, own, other, upper, inverse, work, strip):
    blocks, rows = top.shape[0], top.shape[1]
    for j in range(blocks):
        for k in range(blocks):
            tile = top[j, :, k * rows : (k + 1) * rows]
            if j == k:
                tile = tile - own[k]
                for n in range(other.shape[0]):
                    tile = tile - other[n, k]
            work[j, k] = tile
    line = lax.broadcasted_iota(jnp.int32, (rows, rows), 0)
    lane = lax.broadcasted_iota(jnp.int32, (rows, rows), 1)

    def step(k, carry):
        strip[0] = work[k, k]
        strip[1] = jnp.where(line == lane, 1.0, 0.0)
        for q in range(1, blocks):
            strip[1 + q] = work[k, lax.rem(k + q, blocks)]
        factor_strip(strip)
        upper[k, k] = jnp.where(lane >= line, strip[0], 0.0)
        inverse[k, k] = strip[1]
        for q in range(1, blocks):
            j = lax.rem(k + q, blocks)
            ahead = k + q < blocks
            upper[k, j] = jnp.where(ahead, strip[1 + q], 0.0)
            inverse[k, j] = jnp.where(ahead, 0.0, strip[1 + q])
        pieces = [split(strip[1 + q]) for q in range(blocks)]
        rhs = tuple(jnp.concatenate([p[n] for p in pieces], axis=1) for n in range(2))
        for ahead in range(1, blocks):

            @pl.when(k + ahead < blocks)
            def _():
                j = k + ahead
                drop = dot_rows(split(strip[1 + ahead]), rhs)
                work[j, k] = -drop[:, :rows]
                for q in range(1, blocks):
                    at = lax.rem(k + q, blocks)
                    work[j, at] = work[j, at] - drop[:, q * rows : (q + 1) * rows]

        return carry

    lax.fori_loop(0, blocks, step, 0)


def factor(top, own, other):
    blocks, rows = top.shape[0], top.shape[1]
    square = jax.ShapeDtypeStruct((blocks, blocks, rows, rows), jnp.float32)
    return pl.pallas_call(
        factor_kernel,
        out_shape=(square, square),
        in_specs=[pl.BlockSpec(memory_space=pltpu.VMEM)] * 3,
        out_specs=(pl.BlockSpec(memory_space=pltpu.VMEM),) * 2,
        scratch_shapes=[
            pltpu.VMEM((blocks, blocks, rows, rows), jnp.float32),
            pltpu.VMEM((blocks + 1, rows, rows), jnp.float32),
        ],
        cost_estimate=pl.CostEstimate(
            flops=2 * (blocks * rows) ** 3, bytes_accessed=64 * 1024 * 1024, transcendentals=0
        ),
        name="factor",
    )(top, own, other)


def update_kernel(me, codes, panels, diag, kept, sent):
    leaves = codes.shape[1]
    rows = panels.shape[2]
    per_dest = kept.shape[0]
    half = sent.shape[0] + 1
    blk_count = half * PAIR
    position_count = (per_dest + 1) * blk_count
    block_count = panels.shape[1] // rows
    diag[...] = jnp.zeros_like(diag)
    kept[...] = jnp.zeros_like(kept)
    sent[...] = jnp.zeros_like(sent)

    def absorb(s, carry):
        leaf = lax.div(s, SLOTS)
        at = lax.rem(s, SLOTS) * block_count
        column = codes[leaf, at]

        @pl.when(column < position_count)
        def _():
            panel = panels[s]
            product = lax.dot_general(
                panel,
                panel[:rows],
                (((1,), (1,)), ((), ())),
                preferred_element_type=jnp.float32,
            )
            diag[column] += product[:rows]
            for r in range(1, block_count):
                place = codes[leaf, at + r]
                away = lax.rem(place, blk_count) + blk_count - me[0]
                step = lax.rem(lax.div(away, PAIR), half)
                index = lax.div(place, blk_count) - 1
                inside = (lax.rem(away, PAIR) == 0) & (place < position_count)
                block = product[r * rows : (r + 1) * rows]

                @pl.when(inside & (step == 0))
                def _():
                    kept[index, column] += block

                @pl.when(inside & (step > 0))
                def _():
                    sent[step - 1, index, column] += block

        return carry

    lax.fori_loop(0, panels.shape[0], absorb, 0)


def local_update(me, codes, panels, blk_count, columns, per_dest):
    rows = panels.shape[2]
    smem = pl.BlockSpec(memory_space=pltpu.SMEM)
    vmem = pl.BlockSpec(memory_space=pltpu.VMEM)
    tiles = (per_dest, columns, rows, rows)
    return pl.pallas_call(
        update_kernel,
        out_shape=(
            jax.ShapeDtypeStruct((columns, rows, rows), jnp.float32),
            jax.ShapeDtypeStruct(tiles, jnp.float32),
            jax.ShapeDtypeStruct((blk_count // PAIR - 1,) + tiles, jnp.float32),
        ),
        in_specs=[smem, smem, vmem],
        out_specs=(vmem, vmem, vmem),
        cost_estimate=pl.CostEstimate(
            flops=2 * panels.size * rows, bytes_accessed=4 * panels.size, transcendentals=0
        ),
        name="update",
    )(me, codes, panels)


def exchange_kernel(rows_in, codes_in, top_in, rows_out, codes_out, tops_out, sems, top_sems, local):
    leaves = rows_in.shape[0]
    blks = tops_out.shape[0]
    leaf = lax.axis_index("leaf")
    blk = lax.axis_index("blk")
    mate = blk + 1 - 2 * lax.rem(blk, PAIR)
    MESH = pl.DeviceIdType.MESH

    barrier = pltpu.get_barrier_semaphore()

    def greet_leaf(s, carry):
        pl.semaphore_signal(
            barrier, inc=1, device_id=(lax.rem(leaf + s, leaves), blk), device_id_type=MESH
        )
        return carry

    def greet_blk(s, carry):
        pl.semaphore_signal(
            barrier, inc=1, device_id=(leaf, lax.rem(blk + s, blks)), device_id_type=MESH
        )
        return carry

    lax.fori_loop(1, leaves, greet_leaf, 0)
    lax.fori_loop(1, blks, greet_blk, 0)
    pl.semaphore_wait(barrier, leaves + blks - 2)

    def remote(src, dst, kind, s, leaf_to, blk_to):
        return pltpu.make_async_remote_copy(
            src_ref=src,
            dst_ref=dst,
            send_sem=sems.at[kind, 0, s],
            recv_sem=sems.at[kind, 1, s],
            device_id=(leaf_to, blk_to),
            device_id_type=MESH,
        )

    def outward(s):
        to = lax.rem(leaf + s, leaves)
        return (
            remote(rows_in.at[to], rows_out.at[0, leaf], 0, s, to, blk),
            remote(codes_in.at[to], codes_out.at[0, leaf], 1, s, to, blk),
        )

    def relay(s):
        came = lax.rem(leaf + leaves - s, leaves)
        return (
            remote(rows_out.at[0, came], rows_out.at[1, came], 2, s, leaf, mate),
            remote(codes_out.at[0, came], codes_out.at[1, came], 3, s, leaf, mate),
        )

    def relay_own():
        return (
            remote(rows_in.at[leaf], rows_out.at[1, leaf], 2, 0, leaf, mate),
            remote(codes_in.at[leaf], codes_out.at[1, leaf], 3, 0, leaf, mate),
        )

    def top_copy(s):
        return pltpu.make_async_remote_copy(
            src_ref=top_in,
            dst_ref=tops_out.at[blk],
            send_sem=top_sems.at[0, s],
            recv_sem=top_sems.at[1, s],
            device_id=(leaf, lax.rem(blk + s, blks)),
            device_id_type=MESH,
        )

    def start(s, carry):
        for copy in outward(s):
            copy.start()
        return carry

    lax.fori_loop(1, leaves, start, 0)
    for s in range(1, blks):
        top_copy(s).start()
    for copy in relay_own():
        copy.start()
    kept = (
        pltpu.make_async_copy(rows_in.at[leaf], rows_out.at[0, leaf], local.at[0]),
        pltpu.make_async_copy(codes_in.at[leaf], codes_out.at[0, leaf], local.at[1]),
        pltpu.make_async_copy(top_in, tops_out.at[blk], local.at[2]),
    )
    for copy in kept:
        copy.start()

    def forward(s, carry):
        for copy in outward(s):
            copy.wait_recv()
        for copy in relay(s):
            copy.start()
        return carry

    lax.fori_loop(1, leaves, forward, 0)
    for copy in kept:
        copy.wait()
    for copy in relay_own():
        copy.wait()
    for s in range(1, blks):
        top_copy(s).wait()

    def drain(s, carry):
        for copy in outward(s):
            copy.wait_send()
        for copy in relay(s):
            copy.wait()
        return carry

    lax.fori_loop(1, leaves, drain, 0)


def exchange(rows, codes, top, blk_count):
    leaves = rows.shape[0]
    vmem = pl.BlockSpec(memory_space=pltpu.VMEM)
    return pl.pallas_call(
        exchange_kernel,
        out_shape=(
            jax.ShapeDtypeStruct((PAIR,) + rows.shape, rows.dtype),
            jax.ShapeDtypeStruct((PAIR,) + codes.shape, codes.dtype),
            jax.ShapeDtypeStruct((blk_count,) + top.shape, top.dtype),
        ),
        in_specs=[vmem] * 3,
        out_specs=(vmem,) * 3,
        scratch_shapes=[
            pltpu.SemaphoreType.DMA((4, 2, leaves)),
            pltpu.SemaphoreType.DMA((2, blk_count)),
            pltpu.SemaphoreType.DMA((3,)),
        ],
        compiler_params=pltpu.CompilerParams(collective_id=0, has_side_effects=True),
        name="exchange",
    )(rows, codes, top)


def finish_kernel(me, panel, own, other, upper, inverse, out):
    per_dest, rows = own.shape[0], own.shape[2]
    blocks = upper.shape[0]
    for k in range(blocks):
        tile = upper[k, me[0]]
        out[0, :, k * rows : (k + 1) * rows] = tile.T
    left = []
    for i in range(per_dest):
        parts = []
        for k in range(blocks):
            tile = panel[i + 1, :, k * rows : (k + 1) * rows] - own[i, k]
            for n in range(other.shape[0]):
                tile = tile - other[n, i, k]
            parts.append(tile)
        left.append(jnp.concatenate(parts, axis=1))
    whole_hi, whole_lo = split(jnp.concatenate(left, axis=0))
    for k in range(blocks):
        wide = (k + 1) * rows
        right = jnp.concatenate([inverse[k, q] for q in range(k + 1)], axis=1)
        right_hi, right_lo = split(right)

        def times(x, y):
            return lax.dot_general(
                x, y, (((1,), (1,)), ((), ())), preferred_element_type=jnp.float32
            )

        solved = (
            times(whole_hi[:, :wide], right_hi)
            + times(whole_lo[:, :wide], right_hi)
            + times(whole_hi[:, :wide], right_lo)
        )
        for i in range(per_dest):
            out[i + 1, :, k * rows : (k + 1) * rows] = solved[i * rows : (i + 1) * rows]


def finish(me, panel, own, other, upper, inverse):
    smem = pl.BlockSpec(memory_space=pltpu.SMEM)
    vmem = pl.BlockSpec(memory_space=pltpu.VMEM)
    return pl.pallas_call(
        finish_kernel,
        out_shape=jax.ShapeDtypeStruct(panel.shape, panel.dtype),
        in_specs=[smem] + [vmem] * 5,
        out_specs=vmem,
        cost_estimate=pl.CostEstimate(
            flops=6 * panel.size * panel.shape[2], bytes_accessed=8 * panel.size, transcendentals=0
        ),
        name="finish",
    )(me, panel, own, other, upper, inverse)


def leaf_owner(ranges, anc_order):
    leaves = jnp.arange(anc_order.shape[0], dtype=jnp.int32)
    return jnp.sum(jnp.where(anc_order[None, :] == ranges[:, None], leaves[None, :], 0), axis=1)


def block_positions(block_ids, owner_leaf, anc_order, anc_below, column_blocks, position_count):
    column_base = anc_order[owner_leaf] * column_blocks
    relative = block_ids - column_base[:, None]
    in_columns = (relative >= 0) & (relative < column_blocks)
    below_ids = anc_below[owner_leaf]
    matching = block_ids[:, :, None] == below_ids[:, None, :]
    offsets = column_blocks + jnp.arange(below_ids.shape[1], dtype=jnp.int32)
    below_place = jnp.sum(jnp.where(matching, offsets[None, None, :], 0), axis=2)
    located = jnp.any(matching, axis=2)
    return jnp.where(in_columns, relative, jnp.where(located, below_place, position_count))


def shards(desc_panel, row_map, anc_order, anc_below, anc_panel):
    leaf_count = lax.axis_size("leaf")
    blk_count = lax.axis_size("blk")
    desc_count, block_count = row_map.shape
    block_rows = anc_panel.shape[3]
    panel_width = anc_panel.shape[4]
    wide_desc = desc_panel.shape[2]
    column_blocks = panel_width // block_rows
    position_count = column_blocks + anc_below.shape[1]
    if column_blocks != blk_count or blk_count % PAIR or wide_desc != block_rows:
        raise ValueError("unsupported sizes")
    slot_count = leaf_count * SLOTS
    mine = lax.axis_index("blk")
    me = mine.astype(jnp.int32).reshape(1)
    local_rows = anc_panel.reshape(anc_panel.shape[1], block_rows, panel_width)

    owner_leaf = leaf_owner(row_map[:, 0] // column_blocks, anc_order)
    positions = block_positions(
        row_map, owner_leaf, anc_order, anc_below, column_blocks, position_count
    )
    desc_index = jnp.arange(desc_count, dtype=jnp.int32)
    same_owner = owner_leaf[:, None] == owner_leaf[None, :]
    earlier = desc_index[None, :] < desc_index[:, None]
    ranking = jnp.sum(same_owner & earlier, axis=1)
    slot_of = owner_leaf * SLOTS + ranking
    matches = slot_of[None, :] == jnp.arange(slot_count, dtype=jnp.int32)[:, None]
    filled = jnp.any(matches, axis=1)
    chosen = jnp.sum(jnp.where(matches, desc_index[None, :], 0), axis=1)
    slot_codes = jnp.where(filled[:, None], positions[chosen], position_count)
    slot_codes = slot_codes.reshape(leaf_count, 1, SLOTS * block_count)
    slot_codes = jnp.pad(slot_codes, ((0, 0), (0, 0), (0, 128 - SLOTS * block_count)))
    send_rows = jnp.take(desc_panel, chosen, axis=0)
    send_rows = send_rows.reshape(leaf_count, SLOTS * block_count * block_rows, wide_desc)
    panels, codes, top = exchange(send_rows, slot_codes.astype(jnp.int32), local_rows[0], blk_count)
    panels = panels.reshape(PAIR * slot_count, block_count * block_rows, wide_desc)
    codes = codes.reshape(PAIR * leaf_count, 128)

    per_dest = local_rows.shape[0] - 1
    diag, kept, sent = local_update(me, codes, panels, blk_count, column_blocks, per_dest)

    def shift(x, by):
        return lax.ppermute(x, "blk", [(b, (b + by) % blk_count) for b in range(blk_count)])

    steps = range(1, blk_count // PAIR)
    other_diag = jnp.stack([shift(diag, PAIR * s) for s in steps])
    other_diag, sent = lax.optimization_barrier((other_diag, sent))
    other_below = jnp.stack([shift(sent[s - 1], PAIR * s) for s in steps])
    upper, inverse = factor(top, diag, other_diag)
    out = finish(me, local_rows, kept, other_below, upper, inverse)
    return out.reshape(anc_panel.shape)


def solution(mesh):
    in_specs = (
        P(("leaf", "blk"), None, None),
        P(("leaf", "blk"), None),
        P(),
        P(),
        P("leaf", None, "blk", None, None),
    )
    out_specs = P("leaf", None, "blk", None, None)
    return jax.shard_map(shards, mesh=mesh, in_specs=in_specs, out_specs=out_specs, check_vma=False)
```

```python
import jax
import jax.numpy as jnp
from jax import lax
from jax.experimental import pallas as pl
from jax.experimental.pallas import tpu as pltpu
from jax.sharding import PartitionSpec as P

SLOTS = 2
PAIR = 2

GROUP = 16


def split(x):
    hi = x.astype(jnp.bfloat16)
    return hi, (x - hi.astype(jnp.float32)).astype(jnp.bfloat16)


def dot_rows(lhs, rhs):
    lhs_hi, lhs_lo = lhs
    rhs_hi, rhs_lo = rhs
    return lax.dot_general(
        jnp.concatenate([lhs_hi, lhs_lo, lhs_hi], axis=0),
        jnp.concatenate([rhs_hi, rhs_hi, rhs_lo], axis=0),
        (((0,), (0,)), ((), ())),
        preferred_element_type=jnp.float32,
    )


def factor_strip(strip):
    tiles, rows, _ = strip.shape
    sub = lax.broadcasted_iota(jnp.int32, (GROUP, rows), 0)
    for g in range(rows // GROUP):
        r0 = g * GROUP
        held = [strip[q, r0 : r0 + GROUP, :] for q in range(tiles)]
        cols = [
            jnp.broadcast_to(held[0][:, r0 + t : r0 + t + 1], (GROUP, rows)) for t in range(GROUP)
        ]
        scale = jnp.zeros((GROUP, rows), jnp.float32)
        for t in range(GROUP):
            root = lax.rsqrt(cols[t][t : t + 1, :])
            scale = jnp.where(sub == t, root, scale)
            if t < GROUP - 1:
                mult = jnp.where(sub > t, cols[t], 0.0) * (root * root)
                for u in range(t + 1, GROUP):
                    cols[u] = cols[u] - mult * cols[u][t : t + 1, :]
                held = [h - mult * h[t : t + 1, :] for h in held]
        held = [h * scale for h in held]
        for q in range(tiles):
            strip[q, r0 : r0 + GROUP, :] = held[q]
        if r0 + GROUP < rows:
            pieces = [split(h) for h in held]
            rhs = tuple(jnp.concatenate([p[n] for p in pieces], axis=1) for n in range(2))
            drop = dot_rows(pieces[0], rhs)
            for q in range(tiles):
                strip[q, r0 + GROUP :, :] = (
                    strip[q, r0 + GROUP :, :] - drop[r0 + GROUP :, q * rows : (q + 1) * rows]
                )


def factor_kernel(top, own, upper, inverse, work, strip):
    blocks, rows = top.shape[0], top.shape[1]
    for j in range(blocks):
        for k in range(blocks):
            tile = top[j, :, k * rows : (k + 1) * rows]
            if j == k:
                tile = tile - own[k]
            work[j, k] = tile
    line = lax.broadcasted_iota(jnp.int32, (rows, rows), 0)
    lane = lax.broadcasted_iota(jnp.int32, (rows, rows), 1)

    def step(k, carry):
        strip[0] = work[k, k]
        strip[1] = jnp.where(line == lane, 1.0, 0.0)
        for q in range(1, blocks):
            strip[1 + q] = work[k, lax.rem(k + q, blocks)]
        factor_strip(strip)
        upper[k, k] = jnp.where(lane >= line, strip[0], 0.0)
        inverse[k, k] = strip[1]
        for q in range(1, blocks):
            j = lax.rem(k + q, blocks)
            ahead = k + q < blocks
            upper[k, j] = jnp.where(ahead, strip[1 + q], 0.0)
            inverse[k, j] = jnp.where(ahead, 0.0, strip[1 + q])
        pieces = [split(strip[1 + q]) for q in range(blocks)]
        rhs = tuple(jnp.concatenate([p[n] for p in pieces], axis=1) for n in range(2))
        for ahead in range(1, blocks):

            @pl.when(k + ahead < blocks)
            def _():
                j = k + ahead
                drop = dot_rows(split(strip[1 + ahead]), rhs)
                work[j, k] = -drop[:, :rows]
                for q in range(1, blocks):
                    at = lax.rem(k + q, blocks)
                    work[j, at] = work[j, at] - drop[:, q * rows : (q + 1) * rows]

        return carry

    lax.fori_loop(0, blocks, step, 0)


def factor(top, own):
    blocks, rows = top.shape[0], top.shape[1]
    square = jax.ShapeDtypeStruct((blocks, blocks, rows, rows), jnp.float32)
    return pl.pallas_call(
        factor_kernel,
        out_shape=(square, square),
        in_specs=[pl.BlockSpec(memory_space=pltpu.VMEM)] * 2,
        out_specs=(pl.BlockSpec(memory_space=pltpu.VMEM),) * 2,
        scratch_shapes=[
            pltpu.VMEM((blocks, blocks, rows, rows), jnp.float32),
            pltpu.VMEM((blocks + 1, rows, rows), jnp.float32),
        ],
        cost_estimate=pl.CostEstimate(
            flops=2 * (blocks * rows) ** 3, bytes_accessed=64 * 1024 * 1024, transcendentals=0
        ),
        name="factor",
    )(top, own)


def pack_kernel(row_map, anc_order, anc_below, panels, heads, tails, codes, count):
    desc_count, block_count = row_map.shape
    leaves, below_count = anc_below.shape
    rows = heads.shape[2]
    columns = count.shape[0] // leaves
    position_count = columns + below_count
    heads[...] = jnp.zeros_like(heads)
    tails[...] = jnp.zeros_like(tails)

    def clear(leaf, carry):
        count[leaf] = 0
        for at in range(SLOTS * block_count):
            codes[leaf, at] = position_count
        return carry

    lax.fori_loop(0, leaves, clear, 0)

    def put(d, carry):
        head = row_map[d, 0]
        group = lax.div(head, columns)
        owner = lax.fori_loop(
            0,
            leaves,
            lambda leaf, best: jnp.where(anc_order[leaf] == group, leaf, best),
            0,
            unroll=leaves <= 16,
        )
        slot = count[owner]
        count[owner] = slot + 1
        at = slot * block_count
        codes[owner, at] = head - group * columns
        for r in range(1, block_count):
            block = row_map[d, r]
            place = position_count
            for q in range(below_count):
                place = jnp.where(anc_below[owner, q] == block, columns + q, place)
            codes[owner, at + r] = place
        heads[owner, slot] = panels[d, :rows]
        tails[owner, slot] = panels[d, rows:]
        return carry

    lax.fori_loop(0, desc_count, put, 0)


def pack(row_map, anc_order, anc_below, panels, columns, rows):
    leaves = anc_order.shape[0]
    wide = panels.shape[2]
    smem = pl.BlockSpec(memory_space=pltpu.SMEM)
    vmem = pl.BlockSpec(memory_space=pltpu.VMEM)
    return pl.pallas_call(
        pack_kernel,
        out_shape=(
            jax.ShapeDtypeStruct((leaves, SLOTS, rows, wide), panels.dtype),
            jax.ShapeDtypeStruct((leaves, SLOTS, panels.shape[1] - rows, wide), panels.dtype),
            jax.ShapeDtypeStruct((leaves, 128), jnp.int32),
        ),
        in_specs=[smem, smem, smem, vmem],
        out_specs=(vmem, vmem, smem),
        scratch_shapes=[pltpu.SMEM((leaves * columns,), jnp.int32)],
        name="pack",
    )(row_map, anc_order, anc_below, panels)


def update_kernel(me, codes, heads, tails, diag, kept):
    step = pl.program_id(0)
    leaves = heads.shape[0]
    rows = heads.shape[2]
    per_dest, columns = kept.shape[0], kept.shape[1]
    blk_count = columns
    position_count = (per_dest + 1) * blk_count
    block_count = 1 + tails.shape[2] // rows

    @pl.when(step == 0)
    def _():
        diag[...] = jnp.zeros_like(diag)
        kept[...] = jnp.zeros_like(kept)

    def absorb(s, carry):
        leaf = lax.div(s, SLOTS)
        slot = lax.rem(s, SLOTS)
        line = step * leaves + leaf
        at = slot * block_count
        column = codes[line, at]

        @pl.when(column < position_count)
        def _():
            head = heads[leaf, slot]

            def times(x):
                return lax.dot_general(
                    x, head, (((1,), (1,)), ((), ())), preferred_element_type=jnp.float32
                )

            diag[column] += times(head)
            for r in range(1, block_count):
                place = codes[line, at + r]
                index = lax.div(place, blk_count) - 1

                @pl.when((lax.rem(place, blk_count) == me[0]) & (place < position_count))
                def _():
                    kept[index, column] += times(tails[leaf, slot, (r - 1) * rows : r * rows])

        return carry

    lax.fori_loop(0, leaves * SLOTS, absorb, 0)


def local_update(me, codes, heads, tails, columns, per_dest):
    sources, leaves, slots, rows, wide = heads.shape
    smem = pl.BlockSpec(memory_space=pltpu.SMEM)
    chunk = min(leaves, 8)
    steps = sources * leaves // chunk
    heads = heads.reshape((steps, chunk) + heads.shape[2:])
    tails = tails.reshape((steps, chunk) + tails.shape[2:])
    out_shape = (
        jax.ShapeDtypeStruct((columns, rows, rows), jnp.float32),
        jax.ShapeDtypeStruct((per_dest, columns, rows, rows), jnp.float32),
    )
    return pl.pallas_call(
        update_kernel,
        grid=(steps,),
        out_shape=out_shape,
        in_specs=[
            smem,
            smem,
            pl.BlockSpec((None,) + heads.shape[1:], lambda i: (i, 0, 0, 0, 0)),
            pl.BlockSpec((None,) + tails.shape[1:], lambda i: (i, 0, 0, 0, 0)),
        ],
        out_specs=(
            pl.BlockSpec(out_shape[0].shape, lambda i: (0, 0, 0)),
            pl.BlockSpec(out_shape[1].shape, lambda i: (0, 0, 0, 0)),
        ),
        name="update",
    )(me, codes, heads, tails)


def exchange_kernel(
    heads_in, tails_in, codes_in, top_in, heads, tails, codes, tops, sems, top_sems, local
):
    leaves = heads_in.shape[0]
    blks = tops.shape[0]
    leaf = lax.axis_index("leaf")
    blk = lax.axis_index("blk")
    mate = blk + 1 - 2 * lax.rem(blk, PAIR)
    across = lax.rem(blk + PAIR, blks)
    MESH = pl.DeviceIdType.MESH
    loads = ((codes_in, codes), (heads_in, heads), (tails_in, tails))

    barrier = pltpu.get_barrier_semaphore()

    def greet_leaf(s, carry):
        pl.semaphore_signal(
            barrier, inc=1, device_id=(lax.rem(leaf + s, leaves), blk), device_id_type=MESH
        )
        return carry

    def greet_blk(s, carry):
        pl.semaphore_signal(
            barrier, inc=1, device_id=(leaf, lax.rem(blk + s, blks)), device_id_type=MESH
        )
        return carry

    lax.fori_loop(1, leaves, greet_leaf, 0)
    lax.fori_loop(1, blks, greet_blk, 0)
    pl.semaphore_wait(barrier, leaves + blks - 2)

    def remote(src, dst, load, kind, s, leaf_to, blk_to):
        return pltpu.make_async_remote_copy(
            src_ref=src,
            dst_ref=dst,
            send_sem=sems.at[load, kind, 0, s],
            recv_sem=sems.at[load, kind, 1, s],
            device_id=(leaf_to, blk_to),
            device_id_type=MESH,
        )

    def outward(load, s):
        source, held = loads[load]
        to = lax.rem(leaf + s, leaves)
        return remote(source.at[to], held.at[0, leaf], load, 0, s, to, blk)

    def came(s):
        return lax.rem(leaf + leaves - s, leaves)

    def to_mate(load, s):
        held = loads[load][1]
        return remote(held.at[0, came(s)], held.at[1, came(s)], load, 1, s, leaf, mate)

    def to_across(load, s):
        held = loads[load][1]
        return remote(held.at[0, came(s)], held.at[2, came(s)], load, 2, s, leaf, across)

    def passed_on(load, s):
        held = loads[load][1]
        return remote(held.at[2, came(s)], held.at[3, came(s)], load, 3, s, leaf, mate)

    def own(load):
        source, held = loads[load]
        return (
            remote(source.at[leaf], held.at[1, leaf], load, 1, 0, leaf, mate),
            remote(source.at[leaf], held.at[2, leaf], load, 2, 0, leaf, across),
        )

    def top_copy(s):
        return pltpu.make_async_remote_copy(
            src_ref=top_in,
            dst_ref=tops.at[blk],
            send_sem=top_sems.at[0, s],
            recv_sem=top_sems.at[1, s],
            device_id=(leaf, lax.rem(blk + s, blks)),
            device_id_type=MESH,
        )

    both = ((0, 1), (2,))

    def start(group):
        def one(s, carry):
            for load in group:
                outward(load, s).start()
            return carry

        lax.fori_loop(1, leaves, one, 0)

    start(both[0])
    kept = [
        pltpu.make_async_copy(source.at[leaf], held.at[0, leaf], local.at[load])
        for load, (source, held) in enumerate(loads)
    ]
    kept.append(pltpu.make_async_copy(top_in, tops.at[blk], local.at[len(loads)]))
    for copy in kept:
        copy.start()
    for load in both[0]:
        for copy in own(load):
            copy.start()
    for s in range(1, blks):
        top_copy(s).start()
    start(both[1])
    for load in both[1]:
        for copy in own(load):
            copy.start()

    def forward(group):
        def relay(s, carry):
            @pl.when(s > 0)
            def _():
                for load in group:
                    outward(load, s).wait_recv()
                    to_mate(load, s).start()
                    to_across(load, s).start()

            return carry

        def relay_across(s, carry):
            for load in group:
                to_across(load, s).wait_recv()
                passed_on(load, s).start()
            return carry

        def both_ways(s, carry):
            relay(s, carry)
            return relay_across(s - 1, carry)

        lax.fori_loop(1, leaves, both_ways, 0)
        relay_across(leaves - 1, 0)

    def settle(group):
        def one(s, carry):
            for load in group:
                to_mate(load, s).wait_recv()
                passed_on(load, s).wait_recv()
            return carry

        lax.fori_loop(0, leaves, one, 0)

    forward(both[0])
    settle(both[0])
    forward(both[1])
    settle(both[1])
    for copy in kept:
        copy.wait()
    for s in range(1, blks):
        top_copy(s).wait()
    for group in both:
        for load in group:
            for copy in own(load):
                copy.wait_send()

        def drain(s, carry, group=group):
            for load in group:
                outward(load, s).wait_send()
                to_mate(load, s).wait_send()
                to_across(load, s).wait_send()
            return carry

        def drain_last(s, carry, group=group):
            for load in group:
                passed_on(load, s).wait_send()
            return carry

        lax.fori_loop(1, leaves, drain, 0)
        lax.fori_loop(0, leaves, drain_last, 0)


def exchange(heads, tails, codes, top, blk_count):
    leaves = heads.shape[0]
    small = heads.size + tails.size < 4 * 1024 * 1024
    vmem = pl.BlockSpec(memory_space=pltpu.VMEM if small else pl.ANY)
    return pl.pallas_call(
        exchange_kernel,
        out_shape=tuple(
            jax.ShapeDtypeStruct((blk_count,) + x.shape, x.dtype) for x in (heads, tails, codes, top)
        ),
        in_specs=[vmem] * 4,
        out_specs=(vmem,) * 4,
        scratch_shapes=[
            pltpu.SemaphoreType.DMA((3, 4, 2, leaves)),
            pltpu.SemaphoreType.DMA((2, blk_count)),
            pltpu.SemaphoreType.DMA((4,)),
        ],
        compiler_params=pltpu.CompilerParams(collective_id=0, has_side_effects=True),
        name="exchange",
    )(heads, tails, codes, top)


def finish_kernel(me, panel, own, upper, inverse, out):
    per_dest, rows = own.shape[0], own.shape[2]
    blocks = upper.shape[0]
    for k in range(blocks):
        tile = upper[k, me[0]]
        out[0, :, k * rows : (k + 1) * rows] = tile.T
    left = []
    for i in range(per_dest):
        parts = []
        for k in range(blocks):
            parts.append(panel[i + 1, :, k * rows : (k + 1) * rows] - own[i, k])
        left.append(jnp.concatenate(parts, axis=1))
    whole_hi, whole_lo = split(jnp.concatenate(left, axis=0))
    for k in range(blocks):
        wide = (k + 1) * rows
        right = jnp.concatenate([inverse[k, q] for q in range(k + 1)], axis=1)
        right_hi, right_lo = split(right)

        def times(x, y):
            return lax.dot_general(
                x, y, (((1,), (1,)), ((), ())), preferred_element_type=jnp.float32
            )

        solved = (
            times(whole_hi[:, :wide], right_hi)
            + times(whole_lo[:, :wide], right_hi)
            + times(whole_hi[:, :wide], right_lo)
        )
        for i in range(per_dest):
            out[i + 1, :, k * rows : (k + 1) * rows] = solved[i * rows : (i + 1) * rows]


def finish(me, panel, own, upper, inverse):
    smem = pl.BlockSpec(memory_space=pltpu.SMEM)
    vmem = pl.BlockSpec(memory_space=pltpu.VMEM)
    return pl.pallas_call(
        finish_kernel,
        out_shape=jax.ShapeDtypeStruct(panel.shape, panel.dtype),
        in_specs=[smem] + [vmem] * 4,
        out_specs=vmem,
        cost_estimate=pl.CostEstimate(
            flops=6 * panel.size * panel.shape[2], bytes_accessed=8 * panel.size, transcendentals=0
        ),
        name="finish",
    )(me, panel, own, upper, inverse)


def shards(desc_panel, row_map, anc_order, anc_below, anc_panel):
    blk_count = lax.axis_size("blk")
    block_rows = anc_panel.shape[3]
    panel_width = anc_panel.shape[4]
    column_blocks = panel_width // block_rows
    if column_blocks != blk_count or blk_count != 2 * PAIR:
        raise ValueError("unsupported sizes")
    me = lax.axis_index("blk").astype(jnp.int32).reshape(1)
    local_rows = anc_panel.reshape(anc_panel.shape[1], block_rows, panel_width)
    heads, tails, codes = pack(
        row_map, anc_order, anc_below, desc_panel, column_blocks, block_rows
    )
    codes = codes.reshape(codes.shape[0], 1, codes.shape[1])
    heads, tails, codes, top = exchange(heads, tails, codes, local_rows[0], blk_count)
    codes = codes.reshape(-1, codes.shape[-1])
    diag, kept = local_update(me, codes, heads, tails, column_blocks, local_rows.shape[0] - 1)
    upper, inverse = factor(top, diag)
    out = finish(me, local_rows, kept, upper, inverse)
    return out.reshape(anc_panel.shape)


def solution(mesh):
    in_specs = (
        P(("leaf", "blk"), None, None),
        P(("leaf", "blk"), None),
        P(),
        P(),
        P("leaf", None, "blk", None, None),
    )
    out_specs = P("leaf", None, "blk", None, None)
    return jax.shard_map(shards, mesh=mesh, in_specs=in_specs, out_specs=out_specs, check_vma=False)
```

```python
import functools

import jax
import jax.numpy as jnp
from jax import lax
from jax.experimental import pallas as pl
from jax.experimental.pallas import tpu as pltpu
from jax.sharding import PartitionSpec as P

SLOTS = 2
PAIR = 2

GROUP = 16


def split(x):
    hi = x.astype(jnp.bfloat16)
    return hi, (x - hi.astype(jnp.float32)).astype(jnp.bfloat16)


def dot_rows(lhs, rhs):
    lhs_hi, lhs_lo = lhs
    rhs_hi, rhs_lo = rhs
    return lax.dot_general(
        jnp.concatenate([lhs_hi, lhs_lo, lhs_hi], axis=0),
        jnp.concatenate([rhs_hi, rhs_hi, rhs_lo], axis=0),
        (((0,), (0,)), ((), ())),
        preferred_element_type=jnp.float32,
    )


def factor_strip(strip):
    tiles, rows, _ = strip.shape
    sub = lax.broadcasted_iota(jnp.int32, (GROUP, rows), 0)
    for g in range(rows // GROUP):
        r0 = g * GROUP
        held = [strip[q, r0 : r0 + GROUP, :] for q in range(tiles)]
        cols = [
            jnp.broadcast_to(held[0][:, r0 + t : r0 + t + 1], (GROUP, rows)) for t in range(GROUP)
        ]
        scale = jnp.zeros((GROUP, rows), jnp.float32)
        for t in range(GROUP):
            root = lax.rsqrt(cols[t][t : t + 1, :])
            scale = jnp.where(sub == t, root, scale)
            if t < GROUP - 1:
                mult = jnp.where(sub > t, cols[t], 0.0) * (root * root)
                for u in range(t + 1, GROUP):
                    cols[u] = cols[u] - mult * cols[u][t : t + 1, :]
                held = [h - mult * h[t : t + 1, :] for h in held]
        held = [h * scale for h in held]
        for q in range(tiles):
            strip[q, r0 : r0 + GROUP, :] = held[q]
        if r0 + GROUP < rows:
            pieces = [split(h) for h in held]
            rhs = tuple(jnp.concatenate([p[n] for p in pieces], axis=1) for n in range(2))
            drop = dot_rows(pieces[0], rhs)
            for q in range(tiles):
                strip[q, r0 + GROUP :, :] = (
                    strip[q, r0 + GROUP :, :] - drop[r0 + GROUP :, q * rows : (q + 1) * rows]
                )


def factor_kernel(top, own, other, upper, inverse, work, strip):
    blocks, rows = top.shape[0], top.shape[1]
    for j in range(blocks):
        for k in range(blocks):
            tile = top[j, :, k * rows : (k + 1) * rows]
            if j == k:
                tile = tile - own[k]
                for n in range(other.shape[0]):
                    tile = tile - other[n, k]
            work[j, k] = tile
    line = lax.broadcasted_iota(jnp.int32, (rows, rows), 0)
    lane = lax.broadcasted_iota(jnp.int32, (rows, rows), 1)

    def step(k, carry):
        strip[0] = work[k, k]
        strip[1] = jnp.where(line == lane, 1.0, 0.0)
        for q in range(1, blocks):
            strip[1 + q] = work[k, lax.rem(k + q, blocks)]
        factor_strip(strip)
        upper[k, k] = jnp.where(lane >= line, strip[0], 0.0)
        inverse[k, k] = strip[1]
        for q in range(1, blocks):
            j = lax.rem(k + q, blocks)
            ahead = k + q < blocks
            upper[k, j] = jnp.where(ahead, strip[1 + q], 0.0)
            inverse[k, j] = jnp.where(ahead, 0.0, strip[1 + q])
        pieces = [split(strip[1 + q]) for q in range(blocks)]
        rhs = tuple(jnp.concatenate([p[n] for p in pieces], axis=1) for n in range(2))
        for ahead in range(1, blocks):

            @pl.when(k + ahead < blocks)
            def _():
                j = k + ahead
                drop = dot_rows(split(strip[1 + ahead]), rhs)
                work[j, k] = -drop[:, :rows]
                for q in range(1, blocks):
                    at = lax.rem(k + q, blocks)
                    work[j, at] = work[j, at] - drop[:, q * rows : (q + 1) * rows]

        return carry

    lax.fori_loop(0, blocks, step, 0)


def factor(top, own, other):
    blocks, rows = top.shape[0], top.shape[1]
    square = jax.ShapeDtypeStruct((blocks, blocks, rows, rows), jnp.float32)
    return pl.pallas_call(
        factor_kernel,
        out_shape=(square, square),
        in_specs=[pl.BlockSpec(memory_space=pltpu.VMEM)] * 3,
        out_specs=(pl.BlockSpec(memory_space=pltpu.VMEM),) * 2,
        scratch_shapes=[
            pltpu.VMEM((blocks, blocks, rows, rows), jnp.float32),
            pltpu.VMEM((blocks + 1, rows, rows), jnp.float32),
        ],
        cost_estimate=pl.CostEstimate(
            flops=2 * (blocks * rows) ** 3, bytes_accessed=64 * 1024 * 1024, transcendentals=0
        ),
        name="factor",
    )(top, own, other)


def pack_kernel(row_map, anc_order, anc_below, panels, heads, tails, codes, count):
    desc_count, block_count = row_map.shape
    leaves, below_count = anc_below.shape
    rows = heads.shape[2]
    columns = count.shape[0] // leaves
    position_count = columns + below_count
    heads[...] = jnp.zeros_like(heads)
    tails[...] = jnp.zeros_like(tails)

    def clear(leaf, carry):
        count[leaf] = 0
        for at in range(SLOTS * block_count):
            codes[leaf, at] = position_count
        return carry

    lax.fori_loop(0, leaves, clear, 0)

    def put(d, carry):
        head = row_map[d, 0]
        group = lax.div(head, columns)
        owner = lax.fori_loop(
            0,
            leaves,
            lambda leaf, best: jnp.where(anc_order[leaf] == group, leaf, best),
            0,
            unroll=leaves <= 16,
        )
        slot = count[owner]
        count[owner] = slot + 1
        at = slot * block_count
        codes[owner, at] = head - group * columns
        for r in range(1, block_count):
            block = row_map[d, r]
            place = position_count
            for q in range(below_count):
                place = jnp.where(anc_below[owner, q] == block, columns + q, place)
            codes[owner, at + r] = place
        heads[owner, slot] = panels[d, :rows]
        tails[owner, slot] = panels[d, rows:]
        return carry

    lax.fori_loop(0, desc_count, put, 0)


def pack(row_map, anc_order, anc_below, panels, columns, rows):
    leaves = anc_order.shape[0]
    wide = panels.shape[2]
    smem = pl.BlockSpec(memory_space=pltpu.SMEM)
    vmem = pl.BlockSpec(memory_space=pltpu.VMEM)
    return pl.pallas_call(
        pack_kernel,
        out_shape=(
            jax.ShapeDtypeStruct((leaves, SLOTS, rows, wide), panels.dtype),
            jax.ShapeDtypeStruct((leaves, SLOTS, panels.shape[1] - rows, wide), panels.dtype),
            jax.ShapeDtypeStruct((leaves, 128), jnp.int32),
        ),
        in_specs=[smem, smem, smem, vmem],
        out_specs=(vmem, vmem, smem),
        scratch_shapes=[pltpu.SMEM((leaves * columns,), jnp.int32)],
        name="pack",
    )(row_map, anc_order, anc_below, panels)


def times_head(x, head):
    return lax.dot_general(x, head, (((1,), (1,)), ((), ())), preferred_element_type=jnp.float32)


def diag_kernel(position_count, block_count, codes, heads, diag):
    step = pl.program_id(0)
    leaves = heads.shape[0]

    @pl.when(step == 0)
    def _():
        diag[...] = jnp.zeros_like(diag)

    def absorb(leaf, carry):
        for slot in range(SLOTS):
            column = codes[step * leaves + leaf, slot * block_count]

            @pl.when(column < position_count)
            def _():
                head = heads[leaf, slot]
                diag[column] += times_head(head, head)

        return carry

    lax.fori_loop(0, leaves, absorb, 0)


def below_kernel(me, codes, heads, tails, kept, sent):
    step = pl.program_id(0)
    leaves = heads.shape[0]
    rows = heads.shape[2]
    per_dest = kept.shape[0]
    half = sent.shape[0] + 1
    blk_count = half * PAIR
    position_count = (per_dest + 1) * blk_count
    block_count = 1 + tails.shape[2] // rows

    @pl.when(step == 0)
    def _():
        kept[...] = jnp.zeros_like(kept)
        sent[...] = jnp.zeros_like(sent)

    def absorb(leaf, carry):
        line = step * leaves + leaf
        for slot in range(SLOTS):
            at = slot * block_count
            column = codes[line, at]

            @pl.when(column < position_count)
            def _():
                head = heads[leaf, slot]
                for r in range(1, block_count):
                    place = codes[line, at + r]
                    away = lax.rem(place, blk_count) + blk_count - me[0]
                    hop = lax.rem(lax.div(away, PAIR), half)
                    index = lax.div(place, blk_count) - 1
                    inside = (lax.rem(away, PAIR) == 0) & (place < position_count)

                    def block():
                        return times_head(tails[leaf, slot, (r - 1) * rows : r * rows], head)

                    @pl.when(inside & (hop == 0))
                    def _():
                        kept[index, column] += block()

                    @pl.when(inside & (hop > 0))
                    def _():
                        sent[hop - 1, index, column] += block()

        return carry

    lax.fori_loop(0, leaves, absorb, 0)


def local_update(me, codes, heads, tails, columns, per_dest):
    leaves, rows = heads.shape[1], heads.shape[3]
    smem = pl.BlockSpec(memory_space=pltpu.SMEM)
    chunk = min(leaves, 8)
    steps = heads.shape[0] * leaves // chunk
    block_count = 1 + tails.shape[3] // rows
    heads = heads.reshape((steps, chunk) + heads.shape[2:])
    tails = tails.reshape((steps, chunk) + tails.shape[2:])

    def streamed(x):
        return pl.BlockSpec((None,) + x.shape[1:], lambda i: (i, 0, 0, 0, 0))

    def held(x):
        return pl.BlockSpec(x.shape, lambda i: (0,) * len(x.shape))

    def cost(x):
        return pl.CostEstimate(
            flops=2 * x.size * rows, bytes_accessed=8 * x.size, transcendentals=0
        )

    diag_shape = jax.ShapeDtypeStruct((columns, rows, rows), jnp.float32)
    diag = pl.pallas_call(
        functools.partial(diag_kernel, (per_dest + 1) * columns, block_count),
        grid=(steps,),
        out_shape=diag_shape,
        in_specs=[smem, streamed(heads)],
        out_specs=held(diag_shape),
        cost_estimate=cost(heads),
        name="diag_update",
    )(codes, heads)
    tiles = (per_dest, columns, rows, rows)
    below_shape = (
        jax.ShapeDtypeStruct(tiles, jnp.float32),
        jax.ShapeDtypeStruct((columns // PAIR - 1,) + tiles, jnp.float32),
    )
    kept, sent = pl.pallas_call(
        below_kernel,
        grid=(steps,),
        out_shape=below_shape,
        in_specs=[smem, smem, streamed(heads), streamed(tails)],
        out_specs=tuple(held(x) for x in below_shape),
        cost_estimate=cost(tails),
        name="below_update",
    )(me, codes, heads, tails)
    return diag, kept, sent


def exchange_kernel(
    heads_in, tails_in, codes_in, top_in, heads, tails, codes, tops, sems, top_sems, local
):
    leaves = heads_in.shape[0]
    blks = tops.shape[0]
    leaf = lax.axis_index("leaf")
    blk = lax.axis_index("blk")
    mate = blk + 1 - 2 * lax.rem(blk, PAIR)
    MESH = pl.DeviceIdType.MESH
    loads = ((codes_in, codes), (heads_in, heads), (tails_in, tails))

    barrier = pltpu.get_barrier_semaphore()

    def greet_leaf(s, carry):
        pl.semaphore_signal(
            barrier, inc=1, device_id=(lax.rem(leaf + s, leaves), blk), device_id_type=MESH
        )
        return carry

    def greet_blk(s, carry):
        pl.semaphore_signal(
            barrier, inc=1, device_id=(leaf, lax.rem(blk + s, blks)), device_id_type=MESH
        )
        return carry

    lax.fori_loop(1, leaves, greet_leaf, 0)
    lax.fori_loop(1, blks, greet_blk, 0)
    pl.semaphore_wait(barrier, leaves + blks - 2)

    def remote(src, dst, load, kind, s, leaf_to, blk_to):
        return pltpu.make_async_remote_copy(
            src_ref=src,
            dst_ref=dst,
            send_sem=sems.at[load, kind, 0, s],
            recv_sem=sems.at[load, kind, 1, s],
            device_id=(leaf_to, blk_to),
            device_id_type=MESH,
        )

    def outward(load, s):
        source, held = loads[load]
        to = lax.rem(leaf + s, leaves)
        return remote(source.at[to], held.at[0, leaf], load, 0, s, to, blk)

    def came(s):
        return lax.rem(leaf + leaves - s, leaves)

    def to_mate(load, s):
        held = loads[load][1]
        return remote(held.at[0, came(s)], held.at[1, came(s)], load, 1, s, leaf, mate)

    def own(load):
        source, held = loads[load]
        return (remote(source.at[leaf], held.at[1, leaf], load, 1, 0, leaf, mate),)

    def top_copy(s):
        return pltpu.make_async_remote_copy(
            src_ref=top_in.at[0],
            dst_ref=tops.at[blk],
            send_sem=top_sems.at[0, s],
            recv_sem=top_sems.at[1, s],
            device_id=(leaf, lax.rem(blk + s, blks)),
            device_id_type=MESH,
        )

    both = ((0, 1), (2,))

    def start(group):
        def one(s, carry):
            for load in group:
                outward(load, s).start()
            return carry

        lax.fori_loop(1, leaves, one, 0)

    start(both[0])
    kept = [
        pltpu.make_async_copy(source.at[leaf], held.at[0, leaf], local.at[load])
        for load, (source, held) in enumerate(loads)
    ]
    kept.append(pltpu.make_async_copy(top_in.at[0], tops.at[blk], local.at[len(loads)]))
    for copy in kept:
        copy.start()
    for load in both[0]:
        for copy in own(load):
            copy.start()
    for s in range(1, blks):
        top_copy(s).start()
    start(both[1])
    for load in both[1]:
        for copy in own(load):
            copy.start()

    def forward(group):
        def one(s, carry):
            for load in group:
                outward(load, s).wait_recv()
                to_mate(load, s).start()
            return carry

        lax.fori_loop(1, leaves, one, 0)

    for group in both:
        forward(group)
    for copy in kept:
        copy.wait()
    for s in range(1, blks):
        top_copy(s).wait()
    for group in both:
        for load in group:
            for copy in own(load):
                copy.wait()

        def drain(s, carry, group=group):
            for load in group:
                outward(load, s).wait_send()
                to_mate(load, s).wait()
            return carry

        lax.fori_loop(1, leaves, drain, 0)


def exchange(heads, tails, codes, panel, blk_count):
    leaves = heads.shape[0]
    small = heads.size + tails.size < 4 * 1024 * 1024
    vmem = pl.BlockSpec(memory_space=pltpu.VMEM if small else pl.ANY)
    return pl.pallas_call(
        exchange_kernel,
        out_shape=tuple(
            jax.ShapeDtypeStruct((count,) + x.shape, x.dtype)
            for count, x in ((PAIR, heads), (PAIR, tails), (PAIR, codes))
        )
        + (jax.ShapeDtypeStruct((blk_count,) + panel.shape[1:], panel.dtype),),
        in_specs=[vmem] * 4,
        out_specs=(vmem,) * 4,
        scratch_shapes=[
            pltpu.SemaphoreType.DMA((3, 2, 2, leaves)),
            pltpu.SemaphoreType.DMA((2, blk_count)),
            pltpu.SemaphoreType.DMA((4,)),
        ],
        compiler_params=pltpu.CompilerParams(collective_id=0, has_side_effects=True),
        name="exchange",
    )(heads, tails, codes, panel)


def finish_kernel(me, panel, own, other, upper, inverse, out):
    per_dest, rows = own.shape[0], own.shape[2]
    blocks = upper.shape[0]
    for k in range(blocks):
        tile = upper[k, me[0]]
        out[0, :, k * rows : (k + 1) * rows] = tile.T
    left = []
    for i in range(per_dest):
        parts = []
        for k in range(blocks):
            tile = panel[i + 1, :, k * rows : (k + 1) * rows] - own[i, k]
            for n in range(other.shape[0]):
                tile = tile - other[n, i, k]
            parts.append(tile)
        left.append(jnp.concatenate(parts, axis=1))
    whole_hi, whole_lo = split(jnp.concatenate(left, axis=0))
    for k in range(blocks):
        wide = (k + 1) * rows
        right = jnp.concatenate([inverse[k, q] for q in range(k + 1)], axis=1)
        right_hi, right_lo = split(right)

        def times(x, y):
            return lax.dot_general(
                x, y, (((1,), (1,)), ((), ())), preferred_element_type=jnp.float32
            )

        solved = (
            times(whole_hi[:, :wide], right_hi)
            + times(whole_lo[:, :wide], right_hi)
            + times(whole_hi[:, :wide], right_lo)
        )
        for i in range(per_dest):
            out[i + 1, :, k * rows : (k + 1) * rows] = solved[i * rows : (i + 1) * rows]


def finish(me, panel, own, other, upper, inverse):
    smem = pl.BlockSpec(memory_space=pltpu.SMEM)
    vmem = pl.BlockSpec(memory_space=pltpu.VMEM)
    return pl.pallas_call(
        finish_kernel,
        out_shape=jax.ShapeDtypeStruct(panel.shape, panel.dtype),
        in_specs=[smem] + [vmem] * 5,
        out_specs=vmem,
        cost_estimate=pl.CostEstimate(
            flops=6 * panel.size * panel.shape[2], bytes_accessed=8 * panel.size, transcendentals=0
        ),
        name="finish",
    )(me, panel, own, other, upper, inverse)


def shards(desc_panel, row_map, anc_order, anc_below, anc_panel):
    blk_count = lax.axis_size("blk")
    block_rows = anc_panel.shape[3]
    panel_width = anc_panel.shape[4]
    column_blocks = panel_width // block_rows
    if column_blocks != blk_count or blk_count != 2 * PAIR:
        raise ValueError("unsupported sizes")
    me = lax.axis_index("blk").astype(jnp.int32).reshape(1)
    local_rows = anc_panel.reshape(anc_panel.shape[1], block_rows, panel_width)
    heads, tails, codes = pack(
        row_map, anc_order, anc_below, desc_panel, column_blocks, block_rows
    )
    codes = codes.reshape(codes.shape[0], 1, codes.shape[1])
    heads, tails, codes, top = exchange(heads, tails, codes, local_rows, blk_count)
    codes = codes.reshape(-1, codes.shape[-1])
    diag, kept, sent = local_update(me, codes, heads, tails, column_blocks, local_rows.shape[0] - 1)

    def shift(x, by):
        return lax.ppermute(x, "blk", [(b, (b + by) % blk_count) for b in range(blk_count)])

    hops = range(1, blk_count // PAIR)
    other_diag = jnp.stack([shift(diag, PAIR * s) for s in hops])
    other_diag, sent = lax.optimization_barrier((other_diag, sent))
    other_below = jnp.stack([shift(sent[s - 1], PAIR * s) for s in hops])
    upper, inverse = factor(top, diag, other_diag)
    out = finish(me, local_rows, kept, other_below, upper, inverse)
    return out.reshape(anc_panel.shape)


def solution(mesh):
    in_specs = (
        P(("leaf", "blk"), None, None),
        P(("leaf", "blk"), None),
        P(),
        P(),
        P("leaf", None, "blk", None, None),
    )
    out_specs = P("leaf", None, "blk", None, None)
    return jax.shard_map(shards, mesh=mesh, in_specs=in_specs, out_specs=out_specs, check_vma=False)
```

```python
import functools

import jax
import jax.numpy as jnp
from jax import lax
from jax.experimental import pallas as pl
from jax.experimental.pallas import tpu as pltpu
from jax.sharding import PartitionSpec as P

SLOTS = 2
PAIR = 2

GROUP = 16


def split(x):
    hi = x.astype(jnp.bfloat16)
    return hi, (x - hi.astype(jnp.float32)).astype(jnp.bfloat16)


def dot_rows(lhs, rhs):
    lhs_hi, lhs_lo = lhs
    rhs_hi, rhs_lo = rhs
    return lax.dot_general(
        jnp.concatenate([lhs_hi, lhs_lo, lhs_hi], axis=0),
        jnp.concatenate([rhs_hi, rhs_hi, rhs_lo], axis=0),
        (((0,), (0,)), ((), ())),
        preferred_element_type=jnp.float32,
    )


def factor_strip(strip):
    tiles, rows, _ = strip.shape
    sub = lax.broadcasted_iota(jnp.int32, (GROUP, rows), 0)
    for g in range(rows // GROUP):
        r0 = g * GROUP
        held = [strip[q, r0 : r0 + GROUP, :] for q in range(tiles)]
        cols = [
            jnp.broadcast_to(held[0][:, r0 + t : r0 + t + 1], (GROUP, rows)) for t in range(GROUP)
        ]
        scale = jnp.zeros((GROUP, rows), jnp.float32)
        for t in range(GROUP):
            root = lax.rsqrt(cols[t][t : t + 1, :])
            scale = jnp.where(sub == t, root, scale)
            if t < GROUP - 1:
                mult = jnp.where(sub > t, cols[t], 0.0) * (root * root)
                for u in range(t + 1, GROUP):
                    cols[u] = cols[u] - mult * cols[u][t : t + 1, :]
                held = [h - mult * h[t : t + 1, :] for h in held]
        held = [h * scale for h in held]
        for q in range(tiles):
            strip[q, r0 : r0 + GROUP, :] = held[q]
        if r0 + GROUP < rows:
            pieces = [split(h) for h in held]
            rhs = tuple(jnp.concatenate([p[n] for p in pieces], axis=1) for n in range(2))
            drop = dot_rows(pieces[0], rhs)
            for q in range(tiles):
                strip[q, r0 + GROUP :, :] = (
                    strip[q, r0 + GROUP :, :] - drop[r0 + GROUP :, q * rows : (q + 1) * rows]
                )


def factor_kernel(top, own, other, upper, inverse, work, strip):
    blocks, rows = top.shape[0], top.shape[1]
    for j in range(blocks):
        for k in range(blocks):
            tile = top[j, :, k * rows : (k + 1) * rows]
            if j == k:
                tile = tile - own[k]
                for n in range(other.shape[0]):
                    tile = tile - other[n, k]
            work[j, k] = tile
    line = lax.broadcasted_iota(jnp.int32, (rows, rows), 0)
    lane = lax.broadcasted_iota(jnp.int32, (rows, rows), 1)

    def step(k, carry):
        strip[0] = work[k, k]
        strip[1] = jnp.where(line == lane, 1.0, 0.0)
        for q in range(1, blocks):
            strip[1 + q] = work[k, lax.rem(k + q, blocks)]
        factor_strip(strip)
        upper[k, k] = jnp.where(lane >= line, strip[0], 0.0)
        inverse[k, k] = strip[1]
        for q in range(1, blocks):
            j = lax.rem(k + q, blocks)
            ahead = k + q < blocks
            upper[k, j] = jnp.where(ahead, strip[1 + q], 0.0)
            inverse[k, j] = jnp.where(ahead, 0.0, strip[1 + q])
        pieces = [split(strip[1 + q]) for q in range(blocks)]
        rhs = tuple(jnp.concatenate([p[n] for p in pieces], axis=1) for n in range(2))
        for ahead in range(1, blocks):

            @pl.when(k + ahead < blocks)
            def _():
                j = k + ahead
                drop = dot_rows(split(strip[1 + ahead]), rhs)
                work[j, k] = -drop[:, :rows]
                for q in range(1, blocks):
                    at = lax.rem(k + q, blocks)
                    work[j, at] = work[j, at] - drop[:, q * rows : (q + 1) * rows]

        return carry

    lax.fori_loop(0, blocks, step, 0)


def factor(top, own, other):
    blocks, rows = top.shape[0], top.shape[1]
    square = jax.ShapeDtypeStruct((blocks, blocks, rows, rows), jnp.float32)
    return pl.pallas_call(
        factor_kernel,
        out_shape=(square, square),
        in_specs=[pl.BlockSpec(memory_space=pltpu.VMEM)] * 3,
        out_specs=(pl.BlockSpec(memory_space=pltpu.VMEM),) * 2,
        scratch_shapes=[
            pltpu.VMEM((blocks, blocks, rows, rows), jnp.float32),
            pltpu.VMEM((blocks + 1, rows, rows), jnp.float32),
        ],
        cost_estimate=pl.CostEstimate(
            flops=2 * (blocks * rows) ** 3, bytes_accessed=64 * 1024 * 1024, transcendentals=0
        ),
        name="factor",
    )(top, own, other)


def pack_kernel(row_map, anc_order, anc_below, panels, heads, tails, codes, count):
    desc_count, block_count = row_map.shape
    leaves, below_count = anc_below.shape
    rows = heads.shape[2]
    columns = count.shape[0] // leaves
    position_count = columns + below_count
    heads[...] = jnp.zeros_like(heads)
    tails[...] = jnp.zeros_like(tails)

    def clear(leaf, carry):
        count[leaf] = 0
        for at in range(SLOTS * block_count):
            codes[leaf, at] = position_count
        return carry

    lax.fori_loop(0, leaves, clear, 0)

    def put(d, carry):
        head = row_map[d, 0]
        group = lax.div(head, columns)
        owner = lax.fori_loop(
            0,
            leaves,
            lambda leaf, best: jnp.where(anc_order[leaf] == group, leaf, best),
            0,
            unroll=leaves <= 16,
        )
        slot = count[owner]
        count[owner] = slot + 1
        at = slot * block_count
        codes[owner, at] = head - group * columns
        for r in range(1, block_count):
            block = row_map[d, r]
            place = position_count
            for q in range(below_count):
                place = jnp.where(anc_below[owner, q] == block, columns + q, place)
            codes[owner, at + r] = place
        heads[owner, slot] = panels[d, :rows]
        tails[owner, slot] = panels[d, rows:]
        return carry

    lax.fori_loop(0, desc_count, put, 0)


def pack(row_map, anc_order, anc_below, panels, columns, rows):
    leaves = anc_order.shape[0]
    wide = panels.shape[2]
    smem = pl.BlockSpec(memory_space=pltpu.SMEM)
    vmem = pl.BlockSpec(memory_space=pltpu.VMEM)
    return pl.pallas_call(
        pack_kernel,
        out_shape=(
            jax.ShapeDtypeStruct((leaves, SLOTS, rows, wide), panels.dtype),
            jax.ShapeDtypeStruct((leaves, SLOTS, panels.shape[1] - rows, wide), panels.dtype),
            jax.ShapeDtypeStruct((leaves, 128), jnp.int32),
        ),
        in_specs=[smem, smem, smem, vmem],
        out_specs=(vmem, vmem, smem),
        scratch_shapes=[pltpu.SMEM((leaves * columns,), jnp.int32)],
        name="pack",
    )(row_map, anc_order, anc_below, panels)


def times_head(x, head):
    return lax.dot_general(x, head, (((1,), (1,)), ((), ())), preferred_element_type=jnp.float32)


def diag_kernel(position_count, block_count, codes, heads, diag):
    step = pl.program_id(0)
    leaves = heads.shape[0]

    @pl.when(step == 0)
    def _():
        diag[...] = jnp.zeros_like(diag)

    def absorb(leaf, carry):
        for slot in range(SLOTS):
            column = codes[step * leaves + leaf, slot * block_count]

            @pl.when(column < position_count)
            def _():
                head = heads[leaf, slot]
                diag[column] += times_head(head, head)

        return carry

    lax.fori_loop(0, leaves, absorb, 0)


def below_kernel(me, codes, heads, tails, kept, sent):
    step = pl.program_id(0)
    leaves = heads.shape[0]
    rows = heads.shape[2]
    per_dest = kept.shape[0]
    half = sent.shape[0] + 1
    blk_count = half * PAIR
    position_count = (per_dest + 1) * blk_count
    block_count = 1 + tails.shape[2] // rows

    @pl.when(step == 0)
    def _():
        kept[...] = jnp.zeros_like(kept)
        sent[...] = jnp.zeros_like(sent)

    def absorb(leaf, carry):
        line = step * leaves + leaf
        for slot in range(SLOTS):
            at = slot * block_count
            column = codes[line, at]

            @pl.when(column < position_count)
            def _():
                head = heads[leaf, slot]
                for r in range(1, block_count):
                    place = codes[line, at + r]
                    away = lax.rem(place, blk_count) + blk_count - me[0]
                    hop = lax.rem(lax.div(away, PAIR), half)
                    index = lax.div(place, blk_count) - 1
                    inside = (lax.rem(away, PAIR) == 0) & (place < position_count)

                    def block():
                        return times_head(tails[leaf, slot, (r - 1) * rows : r * rows], head)

                    @pl.when(inside & (hop == 0))
                    def _():
                        kept[index, column] += block()

                    @pl.when(inside & (hop > 0))
                    def _():
                        sent[hop - 1, index, column] += block()

        return carry

    lax.fori_loop(0, leaves, absorb, 0)


def local_update(me, codes, heads, tails, columns, per_dest):
    leaves, rows = heads.shape[1], heads.shape[3]
    smem = pl.BlockSpec(memory_space=pltpu.SMEM)
    chunk = min(leaves, 8)
    steps = heads.shape[0] * leaves // chunk
    block_count = 1 + tails.shape[3] // rows
    heads = heads.reshape((steps, chunk) + heads.shape[2:])
    tails = tails.reshape((steps, chunk) + tails.shape[2:])

    def streamed(x):
        return pl.BlockSpec((None,) + x.shape[1:], lambda i: (i, 0, 0, 0, 0))

    def held(x):
        return pl.BlockSpec(x.shape, lambda i: (0,) * len(x.shape))

    def cost(x):
        return pl.CostEstimate(
            flops=2 * x.size * rows, bytes_accessed=8 * x.size, transcendentals=0
        )

    diag_shape = jax.ShapeDtypeStruct((columns, rows, rows), jnp.float32)
    diag = pl.pallas_call(
        functools.partial(diag_kernel, (per_dest + 1) * columns, block_count),
        grid=(steps,),
        out_shape=diag_shape,
        in_specs=[smem, streamed(heads)],
        out_specs=held(diag_shape),
        cost_estimate=cost(heads),
        name="diag_update",
    )(codes, heads)
    tiles = (per_dest, columns, rows, rows)
    below_shape = (
        jax.ShapeDtypeStruct(tiles, jnp.float32),
        jax.ShapeDtypeStruct((columns // PAIR - 1,) + tiles, jnp.float32),
    )
    kept, sent = pl.pallas_call(
        below_kernel,
        grid=(steps,),
        out_shape=below_shape,
        in_specs=[smem, smem, streamed(heads), streamed(tails)],
        out_specs=tuple(held(x) for x in below_shape),
        cost_estimate=cost(tails),
        name="below_update",
    )(me, codes, heads, tails)
    return diag, kept, sent


def exchange_kernel(
    heads_in, tails_in, codes_in, top_in, heads, tails, codes, tops, sems, top_sems, local
):
    leaves = heads_in.shape[0]
    blks = tops.shape[0]
    leaf = lax.axis_index("leaf")
    blk = lax.axis_index("blk")
    mate = blk + 1 - 2 * lax.rem(blk, PAIR)
    MESH = pl.DeviceIdType.MESH
    loads = ((codes_in, codes), (heads_in, heads), (tails_in, tails))

    barrier = pltpu.get_barrier_semaphore()

    def greet_leaf(s, carry):
        pl.semaphore_signal(
            barrier, inc=1, device_id=(lax.rem(leaf + s, leaves), blk), device_id_type=MESH
        )
        return carry

    def greet_blk(s, carry):
        pl.semaphore_signal(
            barrier, inc=1, device_id=(leaf, lax.rem(blk + s, blks)), device_id_type=MESH
        )
        return carry

    lax.fori_loop(1, leaves, greet_leaf, 0)
    lax.fori_loop(1, blks, greet_blk, 0)
    pl.semaphore_wait(barrier, leaves + blks - 2)

    def remote(src, dst, load, kind, s, leaf_to, blk_to):
        return pltpu.make_async_remote_copy(
            src_ref=src,
            dst_ref=dst,
            send_sem=sems.at[load, kind, 0, s],
            recv_sem=sems.at[load, kind, 1, s],
            device_id=(leaf_to, blk_to),
            device_id_type=MESH,
        )

    def outward(load, s):
        source, held = loads[load]
        to = lax.rem(leaf + s, leaves)
        return remote(source.at[to], held.at[0, leaf], load, 0, s, to, blk)

    def came(s):
        return lax.rem(leaf + leaves - s, leaves)

    def to_mate(load, s):
        held = loads[load][1]
        return remote(held.at[0, came(s)], held.at[1, came(s)], load, 1, s, leaf, mate)

    def own(load):
        source, held = loads[load]
        return (remote(source.at[leaf], held.at[1, leaf], load, 1, 0, leaf, mate),)

    def top_copy(s):
        return pltpu.make_async_remote_copy(
            src_ref=top_in.at[0],
            dst_ref=tops.at[blk],
            send_sem=top_sems.at[0, s],
            recv_sem=top_sems.at[1, s],
            device_id=(leaf, lax.rem(blk + s, blks)),
            device_id_type=MESH,
        )

    both = ((0, 1, 2), ())

    def start(group):
        def one(s, carry):
            for load in group:
                outward(load, s).start()
            return carry

        lax.fori_loop(1, leaves, one, 0)

    start(both[0])
    kept = [
        pltpu.make_async_copy(source.at[leaf], held.at[0, leaf], local.at[load])
        for load, (source, held) in enumerate(loads)
    ]
    kept.append(pltpu.make_async_copy(top_in.at[0], tops.at[blk], local.at[len(loads)]))
    for copy in kept:
        copy.start()
    for load in both[0]:
        for copy in own(load):
            copy.start()
    for s in range(1, blks):
        top_copy(s).start()
    start(both[1])
    for load in both[1]:
        for copy in own(load):
            copy.start()

    def forward(group):
        def one(s, carry):
            for load in group:
                outward(load, s).wait_recv()
                to_mate(load, s).start()
            return carry

        lax.fori_loop(1, leaves, one, 0)

    for group in both:
        forward(group)
    for copy in kept:
        copy.wait()
    for s in range(1, blks):
        top_copy(s).wait()
    for group in both:
        for load in group:
            for copy in own(load):
                copy.wait()

        def drain(s, carry, group=group):
            for load in group:
                outward(load, s).wait_send()
                to_mate(load, s).wait()
            return carry

        lax.fori_loop(1, leaves, drain, 0)


def exchange(heads, tails, codes, panel, blk_count):
    leaves = heads.shape[0]
    small = heads.size + tails.size < 4 * 1024 * 1024
    vmem = pl.BlockSpec(memory_space=pltpu.VMEM if small else pl.ANY)
    return pl.pallas_call(
        exchange_kernel,
        out_shape=tuple(
            jax.ShapeDtypeStruct((count,) + x.shape, x.dtype)
            for count, x in ((PAIR, heads), (PAIR, tails), (PAIR, codes))
        )
        + (jax.ShapeDtypeStruct((blk_count,) + panel.shape[1:], panel.dtype),),
        in_specs=[vmem] * 4,
        out_specs=(vmem,) * 4,
        scratch_shapes=[
            pltpu.SemaphoreType.DMA((3, 2, 2, leaves)),
            pltpu.SemaphoreType.DMA((2, blk_count)),
            pltpu.SemaphoreType.DMA((4,)),
        ],
        compiler_params=pltpu.CompilerParams(collective_id=0, has_side_effects=True),
        name="exchange",
    )(heads, tails, codes, panel)


def finish_kernel(me, panel, own, other, upper, inverse, out):
    per_dest, rows = own.shape[0], own.shape[2]
    blocks = upper.shape[0]
    for k in range(blocks):
        tile = upper[k, me[0]]
        out[0, :, k * rows : (k + 1) * rows] = tile.T
    left = []
    for i in range(per_dest):
        parts = []
        for k in range(blocks):
            tile = panel[i + 1, :, k * rows : (k + 1) * rows] - own[i, k]
            for n in range(other.shape[0]):
                tile = tile - other[n, i, k]
            parts.append(tile)
        left.append(jnp.concatenate(parts, axis=1))
    whole_hi, whole_lo = split(jnp.concatenate(left, axis=0))
    for k in range(blocks):
        wide = (k + 1) * rows
        right = jnp.concatenate([inverse[k, q] for q in range(k + 1)], axis=1)
        right_hi, right_lo = split(right)

        def times(x, y):
            return lax.dot_general(
                x, y, (((1,), (1,)), ((), ())), preferred_element_type=jnp.float32
            )

        solved = (
            times(whole_hi[:, :wide], right_hi)
            + times(whole_lo[:, :wide], right_hi)
            + times(whole_hi[:, :wide], right_lo)
        )
        for i in range(per_dest):
            out[i + 1, :, k * rows : (k + 1) * rows] = solved[i * rows : (i + 1) * rows]


def finish(me, panel, own, other, upper, inverse):
    smem = pl.BlockSpec(memory_space=pltpu.SMEM)
    vmem = pl.BlockSpec(memory_space=pltpu.VMEM)
    return pl.pallas_call(
        finish_kernel,
        out_shape=jax.ShapeDtypeStruct(panel.shape, panel.dtype),
        in_specs=[smem] + [vmem] * 5,
        out_specs=vmem,
        cost_estimate=pl.CostEstimate(
            flops=6 * panel.size * panel.shape[2], bytes_accessed=8 * panel.size, transcendentals=0
        ),
        name="finish",
    )(me, panel, own, other, upper, inverse)


def shards(desc_panel, row_map, anc_order, anc_below, anc_panel):
    blk_count = lax.axis_size("blk")
    block_rows = anc_panel.shape[3]
    panel_width = anc_panel.shape[4]
    column_blocks = panel_width // block_rows
    if column_blocks != blk_count or blk_count != 2 * PAIR:
        raise ValueError("unsupported sizes")
    me = lax.axis_index("blk").astype(jnp.int32).reshape(1)
    local_rows = anc_panel.reshape(anc_panel.shape[1], block_rows, panel_width)
    heads, tails, codes = pack(
        row_map, anc_order, anc_below, desc_panel, column_blocks, block_rows
    )
    codes = codes.reshape(codes.shape[0], 1, codes.shape[1])
    heads, tails, codes, top = exchange(heads, tails, codes, local_rows, blk_count)
    codes = codes.reshape(-1, codes.shape[-1])
    diag, kept, sent = local_update(me, codes, heads, tails, column_blocks, local_rows.shape[0] - 1)

    def shift(x, by):
        return lax.ppermute(x, "blk", [(b, (b + by) % blk_count) for b in range(blk_count)])

    hops = range(1, blk_count // PAIR)
    other_diag = jnp.stack([shift(diag, PAIR * s) for s in hops])
    other_diag, sent = lax.optimization_barrier((other_diag, sent))
    other_below = jnp.stack([shift(sent[s - 1], PAIR * s) for s in hops])
    upper, inverse = factor(top, diag, other_diag)
    out = finish(me, local_rows, kept, other_below, upper, inverse)
    return out.reshape(anc_panel.shape)


def solution(mesh):
    in_specs = (
        P(("leaf", "blk"), None, None),
        P(("leaf", "blk"), None),
        P(),
        P(),
        P("leaf", None, "blk", None, None),
    )
    out_specs = P("leaf", None, "blk", None, None)
    return jax.shard_map(shards, mesh=mesh, in_specs=in_specs, out_specs=out_specs, check_vma=False)
```
